32 devices in a mesh: ta: 2 (over core), gx: 16 (over z, y, x).
Axes of the slice: x: 2, y: 2, z: 4, core: 2. Of those that a mesh axis runs over, the one named last changes fastest.
Arguments:
- time_links: float32 [6, 2, 3, 3, 96, 4608], P('ta', None, None, None, 'gx'), may hold values from -1 to 1, as said below
Outputs:
- loop_planes: float32 [96, 2, 4608], P('gx', None, 'ta')
- correlator: float32 [96, 49], P('gx')
The draws below stay inside these ranges and needn't reach their ends.
Inputs may be any that keep to these rules, and one draw needn't show every extreme that they name: At every site and time, the matrix time_links[t, 0] + i time_links[t, 1] is special unitary.
All inputs are finite; a program needn't handle non-finite values.
Results may differ from the reference program's by a relative error of at most 0.00029.
Values sent between devices are 32-bit elements; how exact they have to be, the bound alone decides.
A program may use at most 64 MiB of HBM per device.

```python
import jax
import jax.numpy as jnp
from jax import lax

NY = 48
NZ = 96
NT = 6
NX = 96
RMAX = 48


def normalize(column_real, column_imag):
    inverse = lax.rsqrt(jnp.sum(column_real * column_real + column_imag * column_imag, axis=0) + 1e-20)
    return (column_real * inverse, column_imag * inverse)


def project(base_real, base_imag, column_real, column_imag):
    inner_real = jnp.sum(base_real * column_real + base_imag * column_imag, axis=0)
    inner_imag = jnp.sum(base_real * column_imag - base_imag * column_real, axis=0)
    new_real = column_real - (base_real * inner_real - base_imag * inner_imag)
    new_imag = column_imag - (base_real * inner_imag + base_imag * inner_real)
    return (new_real, new_imag)


def times_complex(first_real, first_imag, second_real, second_imag):
    return (first_real * second_real - first_imag * second_imag, first_real * second_imag + first_imag * second_real)


def along_planes(innovation, rate):
    keep = jnp.sqrt(1.0 - rate * rate)

    def advance(state, fresh):
        following = rate * state + keep * fresh
        return (following, following)
    first = innovation[0]
    _, rest = lax.scan(advance, first, innovation[1:])
    return jnp.concatenate([first[None], rest], axis=0)


def draw_time_links(key, part):
    base_key = jax.random.fold_in(key, 17)
    noise_key, scale_key, field_key, rate_key, amp_key, white_key = jax.random.split(base_key, 6)
    plane_sites = NY * NZ
    site_shape = (NT, NX, plane_sites)
    noise = jax.random.truncated_normal(noise_key, -4.0, 4.0, (2, 3, 3) + site_shape, jnp.float32)
    innovation = jax.random.truncated_normal(field_key, -4.0, 4.0, (NX, 2, plane_sites), jnp.float32)
    white = jax.random.truncated_normal(white_key, -4.0, 4.0, (2,) + site_shape, jnp.float32)
    strength = jax.random.uniform(scale_key, site_shape, jnp.float32, 4.0, 12.0)
    log_length = jax.random.uniform(rate_key, (plane_sites,), jnp.float32, 0.0, jnp.log(1.0 * NX))
    amplitude = jnp.exp(jax.random.uniform(amp_key, (plane_sites,), jnp.float32, jnp.log(0.4), jnp.log(1.2)))
    rate = jnp.exp(-jnp.exp(-log_length))
    field = along_planes(innovation, rate)
    phase_one = (amplitude * field[:, 0] / NT)[None] + 0.15 * white[0]
    phase_two = (amplitude * field[:, 1] / NT)[None] + 0.15 * white[1]
    phase_three = -(phase_one + phase_two)
    cos_rows = jnp.stack([jnp.cos(phase_one), jnp.cos(phase_two), jnp.cos(phase_three)])
    sin_rows = jnp.stack([jnp.sin(phase_one), jnp.sin(phase_two), jnp.sin(phase_three)])
    unit_matrix = jnp.eye(3, dtype=noise.dtype)[:, :, None, None, None]
    matrix_real = noise[0] + strength[None, None] * unit_matrix * cos_rows[:, None]
    matrix_imag = noise[1] + strength[None, None] * unit_matrix * sin_rows[:, None]
    first_real, first_imag = normalize(matrix_real[:, 0], matrix_imag[:, 0])
    second_real, second_imag = project(first_real, first_imag, matrix_real[:, 1], matrix_imag[:, 1])
    second_real, second_imag = normalize(second_real, second_imag)
    third_real, third_imag = project(first_real, first_imag, matrix_real[:, 2], matrix_imag[:, 2])
    third_real, third_imag = project(second_real, second_imag, third_real, third_imag)
    third_real, third_imag = normalize(third_real, third_imag)
    cross_real = []
    cross_imag = []
    for row_index in range(3):
        next_row = (row_index + 1) % 3
        last_row = (row_index + 2) % 3
        plus_real, plus_imag = times_complex(second_real[next_row], second_imag[next_row], third_real[last_row], third_imag[last_row])
        minus_real, minus_imag = times_complex(second_real[last_row], second_imag[last_row], third_real[next_row], third_imag[next_row])
        cross_real.append(plus_real - minus_real)
        cross_imag.append(plus_imag - minus_imag)
    det_real = jnp.zeros_like(cross_real[0])
    det_imag = jnp.zeros_like(cross_real[0])
    for row_index in range(3):
        term_real, term_imag = times_complex(first_real[row_index], first_imag[row_index], cross_real[row_index], cross_imag[row_index])
        det_real = det_real + term_real
        det_imag = det_imag + term_imag
    fixed_real, fixed_imag = times_complex(third_real, third_imag, det_real, -det_imag)
    whole_real = jnp.stack([first_real, second_real, fixed_real], axis=1)
    whole_imag = jnp.stack([first_imag, second_imag, fixed_imag], axis=1)
    matrix = jnp.stack([whole_real, whole_imag])
    return jnp.transpose(matrix, (3, 0, 1, 2, 4, 5))


def setup_inputs(seed: int = 0) -> dict:
    keys = jax.random.split(jax.random.key(seed), 2)
    return {
        "time_links": draw_time_links(jax.random.fold_in(keys[1], 71), 0),
    }


def complex_mul(left, right):
    terms_real = []
    terms_imag = []
    for middle in range(3):
        left_real = left[0][:, middle:middle + 1]
        left_imag = left[1][:, middle:middle + 1]
        right_real = right[0][middle:middle + 1]
        right_imag = right[1][middle:middle + 1]
        terms_real.append(left_real * right_real - left_imag * right_imag)
        terms_imag.append(left_real * right_imag + left_imag * right_real)
    return jnp.stack([terms_real[0] + terms_real[1] + terms_real[2], terms_imag[0] + terms_imag[1] + terms_imag[2]])


def trace_third(matrix):
    return (matrix[:, 0, 0] + matrix[:, 1, 1] + matrix[:, 2, 2]) / 3.0


def reference(time_links):
    product = time_links[0]
    for slice_index in range(1, NT):
        product = complex_mul(product, time_links[slice_index])
    loop_planes = jnp.transpose(trace_third(product), (1, 0, 2))
    columns = []
    for offset in range(RMAX + 1):
        rolled = jnp.roll(loop_planes, -offset, axis=0)
        columns.append(jnp.sum(loop_planes * rolled, axis=(1, 2)) / (NY * NZ))
    return loop_planes, jnp.stack(columns, axis=1)
```

```python
import functools

import jax
import jax.numpy as jnp
from jax import lax
from jax.experimental import pallas as pl
from jax.experimental.pallas import tpu as pltpu
from jax.sharding import PartitionSpec as P

LANES = 128
SUBLANES = 8
MESH = pl.DeviceIdType.MESH


def cross_conj(first, second):
    row = []
    for k in range(3):
        a, b = (k + 1) % 3, (k + 2) % 3
        ar, ai = first[a]
        br, bi = first[b]
        cr, ci = second[a]
        dr, di = second[b]
        real = (ar * dr - ai * di) - (br * cr - bi * ci)
        imag = (br * ci + bi * cr) - (ar * di + ai * dr)
        row.append((real, imag))
    return row


def row_times(row, matrix):
    out = []
    for k in range(3):
        real = imag = None
        for m in range(3):
            ar, ai = row[m]
            br, bi = matrix[m][k]
            pr = ar * br - ai * bi
            pi = ar * bi + ai * br
            real = pr if real is None else real + pr
            imag = pi if imag is None else imag + pi
        out.append((real, imag))
    return out


def product_rows(load, slices):
    rows = [[load(0, r, c) for c in range(3)] for r in range(2)]
    for t in range(1, slices):
        matrix = [[load(t, r, c) for c in range(3)] for r in range(2)]
        matrix.append(cross_conj(matrix[0], matrix[1]))
        rows = [row_times(row, matrix) for row in rows]
    return rows


def trace_of_product(left, right):
    left = left + [cross_conj(left[0], left[1])]
    right = right + [cross_conj(right[0], right[1])]
    real = imag = None
    for i in range(3):
        for j in range(3):
            ar, ai = left[i][j]
            br, bi = right[j][i]
            pr = ar * br - ai * bi
            pi = ar * bi + ai * br
            real = pr if real is None else real + pr
            imag = pi if imag is None else imag + pi
    return real / 3.0, imag / 3.0


def kernel(
    dims,
    x_ref,
    loop_ref,
    corr_ref,
    xin,
    psend,
    precv,
    tr,
    gath,
    gram,
    part,
    sel,
    in_sem,
    out_sem,
    s1,
    r1,
    s2,
    r2,
    s3,
    r3,
):
    slices, planes, sites, gx_n, chunks, reducers, longest = dims
    half = sites // 2
    chunk = half // chunks
    tiles = chunk // LANES
    per = 2 * half // LANES // reducers
    width = per * LANES
    rp = tr.shape[0]
    wide = gram.shape[1]
    ta = lax.axis_index("ta")
    gx = lax.axis_index("gx")
    other = 1 - ta
    mine = (gx * reducers + gx_n - 1) // gx_n
    is_reducer = jnp.logical_and(mine < reducers, (mine * gx_n) // reducers == gx)

    def in_copy(order, c):
        owner = other if order == 0 else ta
        start = pl.multiple_of(owner * half + c * chunk, LANES)
        slot = order * chunks + c
        return pltpu.make_async_copy(
            x_ref.at[:, pl.ds(0, 2), :, :, :, pl.ds(start, chunk)],
            xin.at[slot],
            in_sem.at[slot],
        )

    for order in range(2):
        for c in range(chunks):
            in_copy(order, c).start()

    barrier = pltpu.get_barrier_semaphore()
    for core in range(2):

        def greet(j, carry, core=core):
            @pl.when(jnp.logical_or(core != ta, j != gx))
            def _():
                pl.semaphore_signal(barrier, inc=1, device_id={"ta": core, "gx": j}, device_id_type=MESH)

            return carry

        lax.fori_loop(0, gx_n, greet, 0)

    tr[...] = jnp.zeros(tr.shape, jnp.float32)

    def loader(slot, lanes):
        def load(t, r, c):
            return tuple(xin[slot, t, r, c, :, q, lanes] for q in range(2))

        return load

    def far_chunk(c):
        in_copy(0, c).wait()
        slot = c

        def tile(i, carry):
            lanes = pl.ds(pl.multiple_of(i * LANES, LANES), LANES)
            rows = product_rows(loader(slot, lanes), slices)
            for r in range(2):
                for k in range(3):
                    for q in range(2):
                        psend[slot, (r * 3 + k) * 2 + q, 0:planes, lanes] = rows[r][k][q]
            return carry

        lax.fori_loop(0, tiles, tile, 0)

    for c in range(chunks):
        far_chunk(c)

    pl.semaphore_wait(barrier, 2 * gx_n - 1)

    def swap(c):
        return pltpu.make_async_remote_copy(
            src_ref=psend.at[c],
            dst_ref=precv.at[c],
            send_sem=s1.at[c],
            recv_sem=r1.at[c],
            device_id={"ta": other, "gx": gx},
            device_id_type=MESH,
        )

    for c in range(chunks):
        swap(c).start()

    def scatter(k, target, sender):
        return pltpu.make_async_remote_copy(
            src_ref=tr.at[:, pl.ds(pl.multiple_of(k * width, LANES), width)],
            dst_ref=gath.at[sender],
            send_sem=s2.at[k],
            recv_sem=r2.at[sender],
            device_id={"ta": ta, "gx": target},
            device_id_type=MESH,
        )

    def out_copy(c, q):
        lanes = pl.ds(pl.multiple_of(q * half + c * chunk, LANES), chunk)
        return pltpu.make_async_copy(
            tr.at[:, lanes],
            loop_ref.at[:, lanes],
            out_sem.at[c * 2 + q],
        )

    def near_chunk(step):
        c = step
        in_copy(1, c).wait()
        swap(c).wait_recv()

        def tile(i, carry):
            lanes = pl.ds(pl.multiple_of(i * LANES, LANES), LANES)
            rows = product_rows(loader(chunks + c, lanes), slices)
            theirs = [
                [
                    tuple(precv[c, (r * 3 + k) * 2 + q, 0:planes, lanes] for q in range(2))
                    for k in range(3)
                ]
                for r in range(2)
            ]
            pair = trace_of_product(rows, theirs)
            for q in range(2):
                place = pl.multiple_of(q * half + c * chunk + i * LANES, LANES)
                tr[0:planes, pl.ds(place, LANES)] = pair[q]
            return carry

        lax.fori_loop(0, tiles, tile, 0)
        for q in range(2):
            out_copy(c, q).start()
            for part_index in range(tiles // per):
                k = q * (reducers // 2) + c * (tiles // per) + part_index
                target = (k * gx_n) // reducers

                @pl.when(target != gx)
                def _():
                    scatter(k, target, gx).start()

                @pl.when(target == gx)
                def _():
                    lanes = pl.ds(pl.multiple_of(k * width, LANES), width)
                    gath[gx] = tr[:, lanes]

    for step in range(chunks):
        near_chunk(step)

    def select(i, carry):
        shape = (wide, sel.shape[2])
        column = lax.broadcasted_iota(jnp.int32, shape, 0)
        separation = lax.broadcasted_iota(jnp.int32, shape, 1)
        within = column % rp
        plane = planes * (column // rp) + within
        away = plane - (planes * gx + i + separation)
        hit = jnp.logical_or(away == 0, away == -planes * gx_n)
        hit = jnp.logical_and(hit, within < planes)
        sel[i] = jnp.where(hit, 1.0, 0.0).astype(jnp.bfloat16)
        return carry

    lax.fori_loop(0, planes, select, 0)

    def report(core, j, slot):
        return pltpu.make_async_remote_copy(
            src_ref=gram.at[pl.ds(pl.multiple_of(j * rp, SUBLANES), rp), :],
            dst_ref=part.at[slot],
            send_sem=s3.at[core * gx_n + j],
            recv_sem=r3.at[slot],
            device_id={"ta": core, "gx": j},
            device_id_type=MESH,
        )

    @pl.when(is_reducer)
    def _():
        def arrive(j, carry):
            @pl.when(j != gx)
            def _():
                scatter(0, gx, j).wait_recv()

            return carry

        lax.fori_loop(0, gx_n, arrive, 0)
        rows = gath[...].reshape(gx_n * rp, width)
        gram[...] = lax.dot_general(
            rows,
            rows,
            (((1,), (1,)), ((), ())),
            precision=lax.Precision.HIGHEST,
            preferred_element_type=jnp.float32,
        )
        slot = ta * reducers + mine
        for core in range(2):

            def tell(j, carry, core=core):
                @pl.when(jnp.logical_or(core != ta, j != gx))
                def _():
                    report(core, j, slot).start()

                return carry

            lax.fori_loop(0, gx_n, tell, 0)
        part[slot] = gram[pl.ds(pl.multiple_of(gx * rp, SUBLANES), rp), :]

    for core in range(2):

        def hear(k, carry, core=core):
            source = (k * gx_n) // reducers

            @pl.when(jnp.logical_or(core != ta, source != gx))
            def _():
                report(core, 0, core * reducers + k).wait_recv()

            return carry

        lax.fori_loop(0, reducers, hear, 0)

    total = jnp.sum(part[...], axis=0)
    high = total.astype(jnp.bfloat16).astype(jnp.float32)
    rest = total - high
    middle = rest.astype(jnp.bfloat16).astype(jnp.float32)
    low = rest - middle
    row_index = lax.broadcasted_iota(jnp.int32, total.shape, 0)
    answer = jnp.zeros((3 * rp, sel.shape[2]), jnp.float32)
    for i in range(planes):
        keep = row_index == i
        pieces = [jnp.where(keep, piece, 0.0) for piece in (high, middle, low)]
        stacked = jnp.concatenate(pieces, axis=0).astype(jnp.bfloat16)
        answer = answer + jnp.dot(stacked, sel[i], preferred_element_type=jnp.float32)
    answer = answer[0:rp] + answer[rp : 2 * rp] + answer[2 * rp : 3 * rp]
    corr_ref[...] = answer[0:planes, 0 : longest + 1] / sites

    for c in range(chunks):
        swap(c).wait_send()
        for q in range(2):
            out_copy(c, q).wait()

    def drain(k, carry):
        @pl.when((k * gx_n) // reducers != gx)
        def _():
            scatter(k, gx, gx).wait_send()

        return carry

    lax.fori_loop(0, reducers, drain, 0)

    @pl.when(is_reducer)
    def _():
        for core in range(2):

            def drain_report(j, carry, core=core):
                @pl.when(jnp.logical_or(core != ta, j != gx))
                def _():
                    report(core, j, 0).wait_send()

                return carry

            lax.fori_loop(0, gx_n, drain_report, 0)


def per_device(gx_n, time_links):
    slices, _, _, _, planes, sites = time_links.shape
    held = time_links.transpose(0, 2, 3, 4, 1, 5)
    half = sites // 2
    longest = planes * (gx_n // 2)
    blocks = half // LANES
    chunks = 3 if blocks % 3 == 0 else 1
    tiles = blocks // chunks
    per = min(p for p in range(1, tiles + 1) if tiles % p == 0 and 2 * blocks // p <= gx_n)
    reducers = 2 * blocks // per
    rp = -(-planes // SUBLANES) * SUBLANES
    wide = gx_n * rp
    chunk = tiles * LANES
    far = -(-(longest + 1) // LANES) * LANES
    dims = (slices, planes, sites, gx_n, chunks, reducers, longest)
    dma = pltpu.SemaphoreType.DMA
    loops, correlator = pl.pallas_call(
        functools.partial(kernel, dims),
        out_shape=(
            jax.ShapeDtypeStruct((rp, sites), jnp.float32),
            jax.ShapeDtypeStruct((planes, longest + 1), jnp.float32),
        ),
        in_specs=[pl.BlockSpec(memory_space=pl.ANY)],
        out_specs=(
            pl.BlockSpec(memory_space=pl.ANY),
            pl.BlockSpec(memory_space=pltpu.VMEM),
        ),
        scratch_shapes=[
            pltpu.VMEM((2 * chunks, slices, 2, 3, planes, 2, chunk), jnp.float32),
            pltpu.VMEM((chunks, 12, rp, chunk), jnp.float32),
            pltpu.VMEM((chunks, 12, rp, chunk), jnp.float32),
            pltpu.VMEM((rp, sites), jnp.float32),
            pltpu.VMEM((gx_n, rp, per * LANES), jnp.float32),
            pltpu.VMEM((wide, wide), jnp.float32),
            pltpu.VMEM((2 * reducers, rp, wide), jnp.float32),
            pltpu.VMEM((planes, wide, far), jnp.bfloat16),
            dma((2 * chunks,)),
            dma((2 * chunks,)),
            dma((chunks,)),
            dma((chunks,)),
            dma((reducers,)),
            dma((gx_n,)),
            dma((2 * gx_n,)),
            dma((2 * reducers,)),
        ],
        compiler_params=pltpu.CompilerParams(collective_id=0, has_side_effects=True),
    )(held)
    return loops[0:planes].reshape(planes, 2, half), correlator


def solution(mesh):
    in_specs = (P("ta", None, None, None, "gx", None),)
    out_specs = (P("gx", None, "ta"), P("gx", None))
    return jax.shard_map(
        functools.partial(per_device, mesh.shape["gx"]),
        mesh=mesh,
        in_specs=in_specs,
        out_specs=out_specs,
        check_vma=False,
    )
```

```python
import functools

import jax
import jax.numpy as jnp
from jax import lax
from jax.experimental import pallas as pl
from jax.experimental.pallas import tpu as pltpu
from jax.sharding import PartitionSpec as P

LANES = 128
SUBLANES = 8
MESH = pl.DeviceIdType.MESH


def cross_conj(first, second):
    row = []
    for k in range(3):
        a, b = (k + 1) % 3, (k + 2) % 3
        ar, ai = first[a]
        br, bi = first[b]
        cr, ci = second[a]
        dr, di = second[b]
        real = (ar * dr - ai * di) - (br * cr - bi * ci)
        imag = (br * ci + bi * cr) - (ar * di + ai * dr)
        row.append((real, imag))
    return row


def row_times(row, matrix):
    out = []
    for k in range(3):
        real = imag = None
        for m in range(3):
            ar, ai = row[m]
            br, bi = matrix[m][k]
            pr = ar * br - ai * bi
            pi = ar * bi + ai * br
            real = pr if real is None else real + pr
            imag = pi if imag is None else imag + pi
        out.append((real, imag))
    return out


def product_rows(load, slices):
    rows = [[load(0, r, c) for c in range(3)] for r in range(2)]
    for t in range(1, slices):
        matrix = [[load(t, r, c) for c in range(3)] for r in range(2)]
        matrix.append(cross_conj(matrix[0], matrix[1]))
        rows = [row_times(row, matrix) for row in rows]
    return rows


def trace_of_product(left, right):
    left = left + [cross_conj(left[0], left[1])]
    right = right + [cross_conj(right[0], right[1])]
    real = imag = None
    for i in range(3):
        for j in range(3):
            ar, ai = left[i][j]
            br, bi = right[j][i]
            pr = ar * br - ai * bi
            pi = ar * bi + ai * br
            real = pr if real is None else real + pr
            imag = pi if imag is None else imag + pi
    return real / 3.0, imag / 3.0


def kernel(
    dims,
    x_ref,
    loop_ref,
    corr_ref,
    xin,
    psend,
    precv,
    tr,
    gath,
    gram,
    part,
    sel,
    in_sem,
    out_sem,
    s1,
    r1,
    s2,
    r2,
    s3,
    r3,
):
    slices, planes, sites, gx_n, chunks, reducers, longest = dims
    half = sites // 2
    chunk = half // chunks
    tiles = chunk // LANES
    per = 2 * half // LANES // reducers
    width = per * LANES
    rp = tr.shape[0]
    wide = gram.shape[1]
    ta = lax.axis_index("ta")
    gx = lax.axis_index("gx")
    other = 1 - ta
    mine = (gx * reducers + gx_n - 1) // gx_n
    is_reducer = jnp.logical_and(mine < reducers, (mine * gx_n) // reducers == gx)

    def in_copy(order, c, i):
        owner = other if order == 0 else ta
        start = pl.multiple_of(owner * half + c * chunk + i * LANES, LANES)
        slot = order * chunks + c
        return pltpu.make_async_copy(
            x_ref.at[:, pl.ds(0, 2), :, :, :, pl.ds(start, LANES)],
            xin.at[slot, :, :, :, :, i],
            in_sem.at[slot, i],
        )

    for order in range(2):
        for c in range(chunks):
            for i in range(tiles):
                in_copy(order, c, i).start()

    barrier = pltpu.get_barrier_semaphore()
    for core in range(2):

        def greet(j, carry, core=core):
            @pl.when(jnp.logical_or(core != ta, j != gx))
            def _():
                pl.semaphore_signal(barrier, inc=1, device_id={"ta": core, "gx": j}, device_id_type=MESH)

            return carry

        lax.fori_loop(0, gx_n, greet, 0)

    tr[...] = jnp.zeros(tr.shape, jnp.float32)

    flat = xin.reshape(*xin.shape[:4], planes * tiles * 2, LANES)

    def loader(slot, i):
        def load(t, r, c):
            return tuple(
                flat[slot, t, r, c, pl.ds(2 * i + q, planes, stride=2 * tiles), :]
                for q in range(2)
            )

        return load

    def far_chunk(c):
        for i in range(tiles):
            in_copy(0, c, i).wait()
        slot = c

        def tile(i, carry):
            lanes = pl.ds(pl.multiple_of(i * LANES, LANES), LANES)
            rows = product_rows(loader(slot, i), slices)
            for r in range(2):
                for k in range(3):
                    for q in range(2):
                        psend[slot, (r * 3 + k) * 2 + q, 0:planes, lanes] = rows[r][k][q]
            return carry

        lax.fori_loop(0, tiles, tile, 0)

    for c in range(chunks):
        far_chunk(c)

    pl.semaphore_wait(barrier, 2 * gx_n - 1)

    def swap(c):
        return pltpu.make_async_remote_copy(
            src_ref=psend.at[c],
            dst_ref=precv.at[c],
            send_sem=s1.at[c],
            recv_sem=r1.at[c],
            device_id={"ta": other, "gx": gx},
            device_id_type=MESH,
        )

    for c in range(chunks):
        swap(c).start()

    def scatter(k, target, sender):
        return pltpu.make_async_remote_copy(
            src_ref=tr.at[:, pl.ds(pl.multiple_of(k * width, LANES), width)],
            dst_ref=gath.at[sender],
            send_sem=s2.at[k],
            recv_sem=r2.at[sender],
            device_id={"ta": ta, "gx": target},
            device_id_type=MESH,
        )

    def out_copy(c, q):
        lanes = pl.ds(pl.multiple_of(q * half + c * chunk, LANES), chunk)
        return pltpu.make_async_copy(
            tr.at[:, lanes],
            loop_ref.at[:, lanes],
            out_sem.at[c * 2 + q],
        )

    def near_chunk(step):
        c = step
        for i in range(tiles):
            in_copy(1, c, i).wait()
        swap(c).wait_recv()

        def tile(i, carry):
            lanes = pl.ds(pl.multiple_of(i * LANES, LANES), LANES)
            rows = product_rows(loader(chunks + c, i), slices)
            theirs = [
                [
                    tuple(precv[c, (r * 3 + k) * 2 + q, 0:planes, lanes] for q in range(2))
                    for k in range(3)
                ]
                for r in range(2)
            ]
            pair = trace_of_product(rows, theirs)
            for q in range(2):
                place = pl.multiple_of(q * half + c * chunk + i * LANES, LANES)
                tr[0:planes, pl.ds(place, LANES)] = pair[q]
            return carry

        lax.fori_loop(0, tiles, tile, 0)
        for q in range(2):
            out_copy(c, q).start()
            for part_index in range(tiles // per):
                k = q * (reducers // 2) + c * (tiles // per) + part_index
                target = (k * gx_n) // reducers

                @pl.when(target != gx)
                def _():
                    scatter(k, target, gx).start()

                @pl.when(target == gx)
                def _():
                    lanes = pl.ds(pl.multiple_of(k * width, LANES), width)
                    gath[gx] = tr[:, lanes]

    for step in range(chunks):
        near_chunk(step)

    def select(i, carry):
        shape = (wide, sel.shape[2])
        column = lax.broadcasted_iota(jnp.int32, shape, 0)
        separation = lax.broadcasted_iota(jnp.int32, shape, 1)
        within = column % rp
        plane = planes * (column // rp) + within
        away = plane - (planes * gx + i + separation)
        hit = jnp.logical_or(away == 0, away == -planes * gx_n)
        hit = jnp.logical_and(hit, within < planes)
        sel[i] = jnp.where(hit, 1.0, 0.0).astype(jnp.bfloat16)
        return carry

    lax.fori_loop(0, planes, select, 0)

    def report(core, j, slot):
        return pltpu.make_async_remote_copy(
            src_ref=gram.at[pl.ds(pl.multiple_of(j * rp, SUBLANES), rp), :],
            dst_ref=part.at[slot],
            send_sem=s3.at[core * gx_n + j],
            recv_sem=r3.at[slot],
            device_id={"ta": core, "gx": j},
            device_id_type=MESH,
        )

    @pl.when(is_reducer)
    def _():
        def arrive(j, carry):
            @pl.when(j != gx)
            def _():
                scatter(0, gx, j).wait_recv()

            return carry

        lax.fori_loop(0, gx_n, arrive, 0)
        rows = gath[...].reshape(gx_n * rp, width)
        gram[...] = lax.dot_general(
            rows,
            rows,
            (((1,), (1,)), ((), ())),
            precision=lax.Precision.HIGHEST,
            preferred_element_type=jnp.float32,
        )
        slot = ta * reducers + mine
        for core in range(2):

            def tell(j, carry, core=core):
                @pl.when(jnp.logical_or(core != ta, j != gx))
                def _():
                    report(core, j, slot).start()

                return carry

            lax.fori_loop(0, gx_n, tell, 0)
        part[slot] = gram[pl.ds(pl.multiple_of(gx * rp, SUBLANES), rp), :]

    for core in range(2):

        def hear(k, carry, core=core):
            source = (k * gx_n) // reducers

            @pl.when(jnp.logical_or(core != ta, source != gx))
            def _():
                report(core, 0, core * reducers + k).wait_recv()

            return carry

        lax.fori_loop(0, reducers, hear, 0)

    total = jnp.sum(part[...], axis=0)
    high = total.astype(jnp.bfloat16).astype(jnp.float32)
    rest = total - high
    middle = rest.astype(jnp.bfloat16).astype(jnp.float32)
    low = rest - middle
    row_index = lax.broadcasted_iota(jnp.int32, total.shape, 0)
    answer = jnp.zeros((3 * rp, sel.shape[2]), jnp.float32)
    for i in range(planes):
        keep = row_index == i
        pieces = [jnp.where(keep, piece, 0.0) for piece in (high, middle, low)]
        stacked = jnp.concatenate(pieces, axis=0).astype(jnp.bfloat16)
        answer = answer + jnp.dot(stacked, sel[i], preferred_element_type=jnp.float32)
    answer = answer[0:rp] + answer[rp : 2 * rp] + answer[2 * rp : 3 * rp]
    corr_ref[...] = answer[0:planes, 0 : longest + 1] / sites

    for c in range(chunks):
        swap(c).wait_send()
        for q in range(2):
            out_copy(c, q).wait()

    def drain(k, carry):
        @pl.when((k * gx_n) // reducers != gx)
        def _():
            scatter(k, gx, gx).wait_send()

        return carry

    lax.fori_loop(0, reducers, drain, 0)

    @pl.when(is_reducer)
    def _():
        for core in range(2):

            def drain_report(j, carry, core=core):
                @pl.when(jnp.logical_or(core != ta, j != gx))
                def _():
                    report(core, j, 0).wait_send()

                return carry

            lax.fori_loop(0, gx_n, drain_report, 0)


def per_device(gx_n, time_links):
    slices, _, _, _, planes, sites = time_links.shape
    held = time_links.transpose(0, 2, 3, 4, 1, 5)
    half = sites // 2
    longest = planes * (gx_n // 2)
    blocks = half // LANES
    chunks = 3 if blocks % 3 == 0 else 1
    tiles = blocks // chunks
    per = min(p for p in range(1, tiles + 1) if tiles % p == 0 and 2 * blocks // p <= gx_n)
    reducers = 2 * blocks // per
    rp = -(-planes // SUBLANES) * SUBLANES
    wide = gx_n * rp
    chunk = tiles * LANES
    far = -(-(longest + 1) // LANES) * LANES
    dims = (slices, planes, sites, gx_n, chunks, reducers, longest)
    dma = pltpu.SemaphoreType.DMA
    loops, correlator = pl.pallas_call(
        functools.partial(kernel, dims),
        out_shape=(
            jax.ShapeDtypeStruct((rp, sites), jnp.float32),
            jax.ShapeDtypeStruct((planes, longest + 1), jnp.float32),
        ),
        in_specs=[pl.BlockSpec(memory_space=pl.ANY)],
        out_specs=(
            pl.BlockSpec(memory_space=pl.ANY),
            pl.BlockSpec(memory_space=pltpu.VMEM),
        ),
        scratch_shapes=[
            pltpu.VMEM((2 * chunks + 1, slices, 2, 3, planes, tiles, 2, LANES), jnp.float32),
            pltpu.VMEM((chunks, 12, rp, chunk), jnp.float32),
            pltpu.VMEM((chunks, 12, rp, chunk), jnp.float32),
            pltpu.VMEM((rp, sites), jnp.float32),
            pltpu.VMEM((gx_n, rp, per * LANES), jnp.float32),
            pltpu.VMEM((wide, wide), jnp.float32),
            pltpu.VMEM((2 * reducers, rp, wide), jnp.float32),
            pltpu.VMEM((planes, wide, far), jnp.bfloat16),
            dma((2 * chunks, tiles)),
            dma((2 * chunks,)),
            dma((chunks,)),
            dma((chunks,)),
            dma((reducers,)),
            dma((gx_n,)),
            dma((2 * gx_n,)),
            dma((2 * reducers,)),
        ],
        compiler_params=pltpu.CompilerParams(collective_id=0, has_side_effects=True),
    )(held)
    return loops[0:planes].reshape(planes, 2, half), correlator


def solution(mesh):
    in_specs = (P("ta", None, None, None, "gx", None),)
    out_specs = (P("gx", None, "ta"), P("gx", None))
    return jax.shard_map(
        functools.partial(per_device, mesh.shape["gx"]),
        mesh=mesh,
        in_specs=in_specs,
        out_specs=out_specs,
        check_vma=False,
    )
```

```python
import functools

import jax
import jax.numpy as jnp
from jax import lax
from jax.experimental import pallas as pl
from jax.experimental.pallas import tpu as pltpu
from jax.sharding import PartitionSpec as P

LANES = 128
SUBLANES = 8
MESH = pl.DeviceIdType.MESH


def cross_conj(first, second):
    row = []
    for k in range(3):
        a, b = (k + 1) % 3, (k + 2) % 3
        ar, ai = first[a]
        br, bi = first[b]
        cr, ci = second[a]
        dr, di = second[b]
        real = (ar * dr - ai * di) - (br * cr - bi * ci)
        imag = (br * ci + bi * cr) - (ar * di + ai * dr)
        row.append((real, imag))
    return row


def row_times(row, matrix):
    out = []
    for k in range(3):
        real = imag = None
        for m in range(3):
            ar, ai = row[m]
            br, bi = matrix[m][k]
            pr = ar * br - ai * bi
            pi = ar * bi + ai * br
            real = pr if real is None else real + pr
            imag = pi if imag is None else imag + pi
        out.append((real, imag))
    return out


def product_rows(load, slices):
    rows = [[load(0, r, c) for c in range(3)] for r in range(2)]
    for t in range(1, slices):
        matrix = [[load(t, r, c) for c in range(3)] for r in range(2)]
        matrix.append(cross_conj(matrix[0], matrix[1]))
        rows = [row_times(row, matrix) for row in rows]
    return rows


def trace_of_product(left, right):
    left = left + [cross_conj(left[0], left[1])]
    right = right + [cross_conj(right[0], right[1])]
    real = imag = None
    for i in range(3):
        for j in range(3):
            ar, ai = left[i][j]
            br, bi = right[j][i]
            pr = ar * br - ai * bi
            pi = ar * bi + ai * br
            real = pr if real is None else real + pr
            imag = pi if imag is None else imag + pi
    return real / 3.0, imag / 3.0


def kernel(
    dims,
    x_ref,
    loop_ref,
    corr_ref,
    xin,
    psend,
    precv,
    tr,
    gath,
    gram,
    part,
    sel,
    in_sem,
    out_sem,
    s1,
    r1,
    s2,
    r2,
    s3,
    r3,
):
    slices, planes, sites, gx_n, chunks, reducers, longest = dims
    half = sites // 2
    chunk = half // chunks
    tiles = chunk // LANES
    per = 2 * half // LANES // reducers
    width = per * LANES
    rp = tr.shape[0]
    wide = gram.shape[1]
    ta = lax.axis_index("ta")
    gx = lax.axis_index("gx")
    other = 1 - ta
    mine = (gx * reducers + gx_n - 1) // gx_n
    is_reducer = jnp.logical_and(mine < reducers, (mine * gx_n) // reducers == gx)

    def in_copy(order, c, i):
        owner = other if order == 0 else ta
        start = pl.multiple_of(owner * half + c * chunk + i * LANES, LANES)
        slot = order * chunks + c
        return pltpu.make_async_copy(
            x_ref.at[:, pl.ds(0, 2), :, :, :, pl.ds(start, LANES)],
            xin.at[slot, :, :, :, :, i],
            in_sem.at[slot, i],
        )

    for order in range(2):
        for c in range(chunks):
            for i in range(tiles):
                in_copy(order, c, i).start()

    barrier = pltpu.get_barrier_semaphore()
    for core in range(2):

        def greet(j, carry, core=core):
            @pl.when(jnp.logical_or(core != ta, j != gx))
            def _():
                pl.semaphore_signal(barrier, inc=1, device_id={"ta": core, "gx": j}, device_id_type=MESH)

            return carry

        lax.fori_loop(0, gx_n, greet, 0)

    tr[...] = jnp.zeros(tr.shape, jnp.float32)

    flat = xin.reshape(*xin.shape[:4], planes * tiles * 2, LANES)

    def loader(slot, i):
        def load(t, r, c):
            return tuple(
                flat[slot, t, r, c, pl.ds(2 * i + q, planes, stride=2 * tiles), :]
                for q in range(2)
            )

        return load

    def far_chunk(c):
        for i in range(tiles):
            in_copy(0, c, i).wait()
        slot = c

        def tile(i, carry):
            lanes = pl.ds(pl.multiple_of(i * LANES, LANES), LANES)
            rows = product_rows(loader(slot, i), slices)
            for r in range(2):
                for k in range(3):
                    for q in range(2):
                        psend[slot, (r * 3 + k) * 2 + q, 0:planes, lanes] = rows[r][k][q]
            return carry

        lax.fori_loop(0, tiles, tile, 0)

    for c in range(chunks):
        far_chunk(c)

    pl.semaphore_wait(barrier, 2 * gx_n - 1)

    def swap(c):
        return pltpu.make_async_remote_copy(
            src_ref=psend.at[c],
            dst_ref=precv.at[c],
            send_sem=s1.at[c],
            recv_sem=r1.at[c],
            device_id={"ta": other, "gx": gx},
            device_id_type=MESH,
        )

    for c in range(chunks):
        swap(c).start()

    def scatter(k, target, sender):
        return pltpu.make_async_remote_copy(
            src_ref=tr.at[:, pl.ds(pl.multiple_of(k * width, LANES), width)],
            dst_ref=gath.at[sender],
            send_sem=s2.at[k],
            recv_sem=r2.at[sender],
            device_id={"ta": ta, "gx": target},
            device_id_type=MESH,
        )

    def out_copy(c, q):
        lanes = pl.ds(pl.multiple_of(q * half + c * chunk, LANES), chunk)
        return pltpu.make_async_copy(
            tr.at[:, lanes],
            loop_ref.at[:, lanes],
            out_sem.at[c * 2 + q],
        )

    def near_chunk(step):
        c = step
        for i in range(tiles):
            in_copy(1, c, i).wait()
        swap(c).wait_recv()

        def tile(i, carry):
            lanes = pl.ds(pl.multiple_of(i * LANES, LANES), LANES)
            rows = product_rows(loader(chunks + c, i), slices)
            theirs = [
                [
                    tuple(precv[c, (r * 3 + k) * 2 + q, 0:planes, lanes] for q in range(2))
                    for k in range(3)
                ]
                for r in range(2)
            ]
            pair = trace_of_product(rows, theirs)
            for q in range(2):
                place = pl.multiple_of(q * half + c * chunk + i * LANES, LANES)
                tr[0:planes, pl.ds(place, LANES)] = pair[q]
            return carry

        lax.fori_loop(0, tiles, tile, 0)
        for q in range(2):
            out_copy(c, q).start()
            for part_index in range(tiles // per):
                k = q * (reducers // 2) + c * (tiles // per) + part_index
                target = (k * gx_n) // reducers

                @pl.when(target != gx)
                def _():
                    scatter(k, target, gx).start()

                @pl.when(target == gx)
                def _():
                    lanes = pl.ds(pl.multiple_of(k * width, LANES), width)
                    gath[gx] = tr[:, lanes]

    for step in range(chunks):
        near_chunk(step)

    def select(i, carry):
        shape = (wide, sel.shape[2])
        column = lax.broadcasted_iota(jnp.int32, shape, 0)
        separation = lax.broadcasted_iota(jnp.int32, shape, 1)
        within = column % rp
        plane = planes * (column // rp) + within
        away = plane - (planes * gx + i + separation)
        hit = jnp.logical_or(away == 0, away == -planes * gx_n)
        hit = jnp.logical_and(hit, within < planes)
        sel[i] = jnp.where(hit, 1.0, 0.0).astype(jnp.bfloat16)
        return carry

    lax.fori_loop(0, planes, select, 0)

    def report(core, j, slot):
        return pltpu.make_async_remote_copy(
            src_ref=gram.at[pl.ds(pl.multiple_of(j * rp, SUBLANES), rp), :],
            dst_ref=part.at[slot],
            send_sem=s3.at[core * gx_n + j],
            recv_sem=r3.at[slot],
            device_id={"ta": core, "gx": j},
            device_id_type=MESH,
        )

    @pl.when(is_reducer)
    def _():
        def arrive(j, carry):
            @pl.when(j != gx)
            def _():
                scatter(0, gx, j).wait_recv()

            return carry

        lax.fori_loop(0, gx_n, arrive, 0)
        rows = gath[...].reshape(gx_n * rp, width)
        gram[...] = lax.dot_general(
            rows,
            rows,
            (((1,), (1,)), ((), ())),
            precision=lax.Precision.HIGHEST,
            preferred_element_type=jnp.float32,
        )
        slot = ta * reducers + mine
        for core in range(2):

            def tell(j, carry, core=core):
                @pl.when(jnp.logical_or(core != ta, j != gx))
                def _():
                    report(core, j, slot).start()

                return carry

            lax.fori_loop(0, gx_n, tell, 0)
        part[slot] = gram[pl.ds(pl.multiple_of(gx * rp, SUBLANES), rp), :]

    for core in range(2):

        def hear(k, carry, core=core):
            source = (k * gx_n) // reducers

            @pl.when(jnp.logical_or(core != ta, source != gx))
            def _():
                report(core, 0, core * reducers + k).wait_recv()

            return carry

        lax.fori_loop(0, reducers, hear, 0)

    total = jnp.sum(part[...], axis=0)
    high = total.astype(jnp.bfloat16).astype(jnp.float32)
    rest = total - high
    middle = rest.astype(jnp.bfloat16).astype(jnp.float32)
    low = rest - middle
    row_index = lax.broadcasted_iota(jnp.int32, total.shape, 0)
    answer = jnp.zeros((3 * rp, sel.shape[2]), jnp.float32)
    for i in range(planes):
        keep = row_index == i
        pieces = [jnp.where(keep, piece, 0.0) for piece in (high, middle, low)]
        stacked = jnp.concatenate(pieces, axis=0).astype(jnp.bfloat16)
        answer = answer + jnp.dot(stacked, sel[i], preferred_element_type=jnp.float32)
    answer = answer[0:rp] + answer[rp : 2 * rp] + answer[2 * rp : 3 * rp]
    corr_ref[...] = answer[0:planes, 0 : longest + 1] / sites

    for c in range(chunks):
        swap(c).wait_send()
        for q in range(2):
            out_copy(c, q).wait()

    def drain(k, carry):
        @pl.when((k * gx_n) // reducers != gx)
        def _():
            scatter(k, gx, gx).wait_send()

        return carry

    lax.fori_loop(0, reducers, drain, 0)

    @pl.when(is_reducer)
    def _():
        for core in range(2):

            def drain_report(j, carry, core=core):
                @pl.when(jnp.logical_or(core != ta, j != gx))
                def _():
                    report(core, j, 0).wait_send()

                return carry

            lax.fori_loop(0, gx_n, drain_report, 0)


def per_device(gx_n, time_links):
    slices, _, _, _, planes, sites = time_links.shape
    held = time_links.transpose(0, 2, 3, 4, 1, 5)
    half = sites // 2
    longest = planes * (gx_n // 2)
    blocks = half // LANES
    chunks = next(c for c in (6, 3, 1) if blocks % c == 0)
    tiles = blocks // chunks
    per = min(p for p in range(1, tiles + 1) if tiles % p == 0 and 2 * blocks // p <= gx_n)
    reducers = 2 * blocks // per
    rp = -(-planes // SUBLANES) * SUBLANES
    wide = gx_n * rp
    chunk = tiles * LANES
    far = -(-(longest + 1) // LANES) * LANES
    dims = (slices, planes, sites, gx_n, chunks, reducers, longest)
    dma = pltpu.SemaphoreType.DMA
    loops, correlator = pl.pallas_call(
        functools.partial(kernel, dims),
        out_shape=(
            jax.ShapeDtypeStruct((rp, sites), jnp.float32),
            jax.ShapeDtypeStruct((planes, longest + 1), jnp.float32),
        ),
        in_specs=[pl.BlockSpec(memory_space=pl.ANY)],
        out_specs=(
            pl.BlockSpec(memory_space=pl.ANY),
            pl.BlockSpec(memory_space=pltpu.VMEM),
        ),
        scratch_shapes=[
            pltpu.VMEM((2 * chunks + 1, slices, 2, 3, planes, tiles, 2, LANES), jnp.float32),
            pltpu.VMEM((chunks, 12, rp, chunk), jnp.float32),
            pltpu.VMEM((chunks, 12, rp, chunk), jnp.float32),
            pltpu.VMEM((rp, sites), jnp.float32),
            pltpu.VMEM((gx_n, rp, per * LANES), jnp.float32),
            pltpu.VMEM((wide, wide), jnp.float32),
            pltpu.VMEM((2 * reducers, rp, wide), jnp.float32),
            pltpu.VMEM((planes, wide, far), jnp.bfloat16),
            dma((2 * chunks, tiles)),
            dma((2 * chunks,)),
            dma((chunks,)),
            dma((chunks,)),
            dma((reducers,)),
            dma((gx_n,)),
            dma((2 * gx_n,)),
            dma((2 * reducers,)),
        ],
        compiler_params=pltpu.CompilerParams(collective_id=0, has_side_effects=True),
    )(held)
    return loops[0:planes].reshape(planes, 2, half), correlator


def solution(mesh):
    in_specs = (P("ta", None, None, None, "gx", None),)
    out_specs = (P("gx", None, "ta"), P("gx", None))
    return jax.shard_map(
        functools.partial(per_device, mesh.shape["gx"]),
        mesh=mesh,
        in_specs=in_specs,
        out_specs=out_specs,
        check_vma=False,
    )
```
